32 devices in a mesh: groups: 2 (over y), seq: 4 (over z), head: 4 (over x, core).
Axes of the slice: x: 2, y: 2, z: 4, core: 2. Of those that a mesh axis runs over, the one named last changes fastest.
Arguments:
- query: bfloat16 [4, 8192], P('groups', 'head'), parts along dimension 0, may hold values from -170 to 170
- cache_keys: bfloat16 [4, 1024, 1024], P('groups', 'seq', 'head'), parts along dimension 0, may hold values from -6 to 6
- cache_values: bfloat16 [4, 1024, 1024], P('groups', 'seq', 'head'), parts along dimension 0, may hold values from -6 to 6
- lengths: int32 [4], P('groups'), parts along dimension 0, may hold values from 256 to 1024
- heavy: int32 [4, 2], P('groups'), parts along dimension 0, may hold values from 0 to 7, as said below
- acc_scores: float32 [4, 8], P('groups', 'seq'), parts along dimension 0, may hold values from 0.01 to 1
- refill_kv: bfloat16 [64, 2, 128, 128], P(('groups', 'seq', 'head')), parts along dimension 0, may hold values from -6 to 6
- refill_dest: int32 [64, 1], P(('groups', 'seq', 'head')), parts along dimension 0, may hold values from 0 to 3, as said below
- refill_req: int32 [64], P(('groups', 'seq', 'head')), parts along dimension 0, may hold values from 0 to 1
- refill_head: int32 [64], P(('groups', 'seq', 'head')), parts along dimension 0, may hold values from 0 to 1
Outputs:
- attn_out: bfloat16 [4, 8192], P('groups'), parts along dimension 0
- block_scores: float32 [4, 8], P('groups', 'seq'), parts along dimension 0
- recalled_kv: bfloat16 [64, 2, 128, 128], P(('groups', 'seq', 'head')), parts along dimension 0
- recall_scores: float32 [32, 2], P(('groups', 'seq', 'head')), parts along dimension 0
The draws below stay inside these ranges and needn't reach their ends.
There are 2 independent parts, one for each index of `groups`. The reference program is written for one: setup_inputs(seed, part) draws one part's arguments, and reference() takes and returns one part's arrays. A program takes and returns all parts, laid end to end along the dimension named above; each array names one. Nothing has to cross between parts.
Inputs may be any that keep to these rules, and one draw needn't show every extreme that they name: `heavy`: the 2 block ids of one request are distinct. `refill_dest`: the block at position j of device (s, h) goes to owner (s + k) mod 4, with k fixed by h and j alone; among the 2 blocks of one device at most 2 name the same owner, and on every device 2 do.
All inputs are finite; a program needn't handle non-finite values.
Results may differ from the reference program's by a relative error of at most 0.0045.
Values may be sent and summed in bfloat16 or wider, within the bound.
A program may use at most 128 MiB of HBM per device.

```python
import math
import jax
import jax.numpy as jnp
from jax import lax

HQ = 64
KVH = 8
DH = 128
BLKTOK = 128
RECENT = 2
BATCH = 2
NBLK = 8
SEQLEN = 1024
NHEAVY = 2
REFILL_DEV = 2
UNITS = 32
N_SEQ = 4
N_HEAD = 4


def lengths_helper(subkey):
    drawn = jax.random.randint(jax.random.fold_in(subkey, 1), (BATCH,), SEQLEN // 4, SEQLEN + 1).astype(jnp.int32)
    fullest = jax.random.randint(jax.random.fold_in(subkey, 2), (), 0, BATCH).astype(jnp.int32)
    return jnp.where(jnp.arange(BATCH, dtype=jnp.int32) == fullest, SEQLEN, drawn).astype(jnp.int32)


def keys_helper(basekey):
    base = jnp.clip(jax.random.normal(jax.random.fold_in(basekey, 12), (BATCH, SEQLEN, KVH * DH), jnp.float32), -6.0, 6.0)
    return base


def draw_lengths(key, part):
    return lengths_helper(jax.random.fold_in(key, 11))


def draw_cache_keys(key, part):
    return keys_helper(key).astype(jnp.bfloat16)


def draw_query(key, part):
    base = jnp.clip(jax.random.normal(jax.random.fold_in(key, 21), (BATCH, HQ, DH), jnp.float32), -6.0, 6.0)
    head_frac = jnp.arange(HQ, dtype=jnp.float32) / (HQ - 1)
    rising = jnp.power(4.0, head_frac)
    base = base * rising[None, :, None]
    return base.reshape(BATCH, HQ * DH).astype(jnp.bfloat16)


def pick_blocks(subkey):
    return jax.random.permutation(subkey, NBLK)[:NHEAVY]


def draw_heavy(key, part):
    subkeys = jax.random.split(jax.random.fold_in(key, 31), BATCH)
    return jax.vmap(pick_blocks)(subkeys).astype(jnp.int32)


def pick_steps(subkey):
    order = jax.random.permutation(subkey, N_SEQ)[:REFILL_DEV]
    return order.at[1].set(order[0])


def draw_refill_dest(key, part):
    subkeys = jax.random.split(jax.random.fold_in(key, 41), N_HEAD)
    steps_table = jax.vmap(pick_steps)(subkeys).astype(jnp.int32)
    unit_ids = jnp.arange(UNITS, dtype=jnp.int32)
    source = unit_ids // REFILL_DEV
    place = unit_ids % REFILL_DEV
    head_dev = source % N_HEAD
    seq_src = source // N_HEAD
    owner = (seq_src + steps_table[head_dev, place]) % N_SEQ
    return owner.astype(jnp.int32).reshape(UNITS, 1)


def place_ends(array, stream_key, smallest, top_value):
    index_at = [jax.random.randint(jax.random.fold_in(stream_key, axis), (), 0, length) for axis, length in enumerate(array.shape)]
    widest = array.shape.index(max(array.shape))
    next_to = index_at[:widest] + [(index_at[widest] + 1) % array.shape[widest]] + index_at[widest + 1:]
    return array.at[tuple(index_at)].set(smallest).at[tuple(next_to)].set(top_value)


def levels(stream_key, extent, pieces, smallest, high):
    loudness, own = 1.0, jax.random.fold_in(stream_key, 6)
    for dim, shards_of in pieces:
        heights = jnp.exp(jax.random.uniform(jax.random.fold_in(own, dim), (shards_of,), jnp.float32, smallest / len(pieces), high / len(pieces)))
        loudness = loudness * jnp.repeat(heights, extent[dim] // shards_of).reshape([-1 if axis == dim else 1 for axis in range(len(extent))])
    return loudness


def scatter_about(rng, dims, scale, reach, cuts=(), held_as=jnp.bfloat16):
    array = jax.random.normal(rng, dims, jnp.float32) * scale
    if len(cuts) > 0:
        array = levels(rng, dims, cuts, -0.22, 0.18) * array
    return jnp.clip(array, min=-reach, max=reach).astype(held_as)


def setup_inputs(seed: int = 0, part: int = 0) -> dict:
    key_of = jax.random.split(jax.random.key(seed), 11)
    part_keys = jax.random.split(jax.random.fold_in(key_of[10], part), 11)
    query = draw_query(jax.random.fold_in(jax.random.fold_in(key_of[10], part), 71), part)
    cache_keys = draw_cache_keys(jax.random.fold_in(jax.random.fold_in(key_of[10], part), 71), part)
    cache_values = scatter_about(part_keys[2], (BATCH, SEQLEN, KVH * DH), 1.0, 6.0, ((1, 4), (2, 4)))
    lengths = draw_lengths(jax.random.fold_in(jax.random.fold_in(key_of[10], part), 71), part)
    heavy = draw_heavy(jax.random.fold_in(jax.random.fold_in(key_of[10], part), 71), part)
    acc_scores = jnp.clip(jnp.exp(math.log(1.0) - 4.6051702 * jax.random.uniform(part_keys[5], (BATCH, NBLK), jnp.float32) ** levels(part_keys[5], (BATCH, NBLK), ((1, 4),), -0.2, 0.2)), 0.01, 1.0)
    refill_kv = scatter_about(part_keys[6], (UNITS, 2, BLKTOK, DH), 1.0, 6.0, ((0, 16),))
    refill_dest = draw_refill_dest(jax.random.fold_in(jax.random.fold_in(key_of[10], part), 71), part)
    refill_req = place_ends(jax.random.randint(part_keys[8], (UNITS,), 0, BATCH), jax.random.fold_in(part_keys[8], 1), 0, BATCH - 1).astype(jnp.int32)
    refill_head = place_ends(jax.random.randint(part_keys[9], (UNITS,), 0, KVH // N_HEAD), jax.random.fold_in(part_keys[9], 1), 0, (KVH // N_HEAD) - 1).astype(jnp.int32)
    return {"query": query, "cache_keys": cache_keys, "cache_values": cache_values, "lengths": lengths, "heavy": heavy, "acc_scores": acc_scores, "refill_kv": refill_kv, "refill_dest": refill_dest, "refill_req": refill_req, "refill_head": refill_head}


def reference(query, cache_keys, cache_values, lengths, heavy, acc_scores, refill_kv, refill_dest, refill_req, refill_head):
    per_group = HQ // KVH
    kv_local = KVH // N_HEAD
    score_scale = 1.0 / math.sqrt(DH)
    hiprec = lax.Precision.HIGHEST
    q_four = query.astype(jnp.float32).reshape(BATCH, KVH, per_group, DH)
    position = jnp.arange(SEQLEN, dtype=jnp.int32)
    block_ids = jnp.arange(NBLK, dtype=jnp.int32)
    heavy_hit = jnp.any(heavy[:, :, None] == block_ids[None, None, :], axis=1)
    recent = block_ids[None, :] >= ((lengths - 1) // BLKTOK - (RECENT - 1))[:, None]
    kept = jnp.repeat(heavy_hit | recent, BLKTOK, axis=1) & (position[None, :] < lengths[:, None])
    keys_four = cache_keys.astype(jnp.float32).reshape(BATCH, SEQLEN, KVH, DH)
    values_four = cache_values.astype(jnp.float32).reshape(BATCH, SEQLEN, KVH, DH)
    scores = jnp.einsum('bkgd,btkd->bkgt', q_four, keys_four, precision=hiprec) * score_scale
    masked = jnp.where(kept[:, None, None, :], scores, -1e+30)
    unit_ids = jnp.arange(UNITS, dtype=jnp.int32)
    source = unit_ids // REFILL_DEV
    place = unit_ids % REFILL_DEV
    head_dev = source % N_HEAD
    unit_kvh = head_dev * kv_local + refill_head
    segment = refill_req * KVH + unit_kvh
    q_units = q_four.reshape(BATCH * KVH, per_group, DH)[segment]
    unit_keys = refill_kv[:, 0].astype(jnp.float32)
    unit_vals = refill_kv[:, 1].astype(jnp.float32)
    unit_scores = jnp.einsum('ugd,urd->ugr', q_units, unit_keys, precision=hiprec) * score_scale
    seg_top = jnp.full((BATCH * KVH, per_group), -1e+30, jnp.float32).at[segment].max(lax.optimization_barrier(jnp.max(unit_scores, axis=2)))
    cache_top = lax.optimization_barrier(jnp.max(masked, axis=3)).reshape(BATCH * KVH, per_group)
    row_top = jnp.maximum(cache_top, seg_top)
    top_four = row_top.reshape(BATCH, KVH, per_group, 1)
    cache_exp = jnp.where(kept[:, None, None, :], jnp.exp(masked - top_four), 0.0)
    unit_exp = jnp.exp(unit_scores - row_top[segment][:, :, None])
    total = lax.optimization_barrier(jnp.sum(cache_exp, axis=3)).reshape(BATCH * KVH, per_group)
    total = total + jax.ops.segment_sum(lax.optimization_barrier(jnp.sum(unit_exp, axis=2)), segment, num_segments=BATCH * KVH)
    cache_wts = lax.optimization_barrier(cache_exp.astype(jnp.bfloat16)).astype(jnp.float32)
    unit_wts = lax.optimization_barrier(unit_exp.astype(jnp.bfloat16)).astype(jnp.float32)
    accum = jnp.einsum('bkgt,btkd->bkgd', cache_wts, values_four, precision=hiprec).reshape(BATCH * KVH, per_group, DH)
    unit_pv = jnp.einsum('ugr,urd->ugd', unit_wts, unit_vals, precision=hiprec)
    accum = accum + jax.ops.segment_sum(unit_pv, segment, num_segments=BATCH * KVH)
    attn_out = (accum / total[:, :, None]).astype(jnp.bfloat16).reshape(BATCH, HQ * DH)
    total_four = total.reshape(BATCH, KVH, per_group, 1)
    token_mass = lax.optimization_barrier(jnp.sum(cache_exp / total_four, axis=(1, 2)))
    block_scores = acc_scores + token_mass.reshape(BATCH, NBLK, BLKTOK).sum(axis=2)
    unit_mass = lax.optimization_barrier(jnp.sum(unit_exp / total[segment][:, :, None], axis=(1, 2)))
    rows_out = refill_dest[:, 0] * N_HEAD + head_dev
    target = rows_out * REFILL_DEV + place
    recalled_kv = jnp.zeros_like(refill_kv).at[target].set(refill_kv)
    recall_scores = jnp.zeros((N_SEQ * N_HEAD, REFILL_DEV), jnp.float32).at[rows_out, place].set(unit_mass)
    return (attn_out, block_scores, recalled_kv, recall_scores)
```

```python
import functools
import math

import jax
import jax.numpy as jnp
from jax import lax
from jax.experimental import pallas as pl
from jax.experimental.pallas import tpu as pltpu
from jax.sharding import PartitionSpec as P

DH = 128
BLKTOK = 128
RECENT = 2
CHUNKS = 4
EARLY = 2
EAGER = 2
LOW_PARITY = 1
ORDER = (1, 0, 3, 2)
SETTLE = (1, 3, 0, 2)
RELAYED = 4
LAST = (1, 3, 0, 2)
VMEM_OUT = 2**20
LANES = 128

NEG_BIG = -1e30


def low_first(chunk):
    return chunk % 2 == LOW_PARITY


def await_all(ref, sem):
    pltpu.make_async_copy(ref, ref, sem.at[0]).wait()


def kernel(
    dims,
    lengths_hbm,
    heavy_hbm,
    dest_hbm,
    req_hbm,
    head_hbm,
    acc_hbm,
    query_hbm,
    keys_hbm,
    values_hbm,
    refill_hbm,
    attn_ref,
    block_ref,
    recalled_ref,
    recall_ref,
    lengths_ref,
    heavy_ref,
    dest_ref,
    req_ref,
    head_ref,
    acc_ref,
    q_buf,
    k_buf,
    v_buf,
    own_kv,
    kv_buf,
    kept_kv,
    part_buf,
    stat_buf,
    mass_buf,
    load_sem,
    kv_send,
    kv_recv,
    part_send,
    part_recv,
    stat_send,
    stat_recv,
    attn_send,
    attn_recv,
    mass_send,
    mass_recv,
    seq_ready,
    head_ready,
):
    n_seq, n_head, masks, chunks = dims
    requests, seq_local = k_buf.shape[0], k_buf.shape[1]
    kv_local = k_buf.shape[2] // DH
    heads_local = q_buf.shape[1] // DH
    per_group = heads_local // kv_local
    rows = requests * heads_local
    blocks_local = seq_local // BLKTOK
    unit_rows = 2 * BLKTOK
    held = own_kv.shape[0] // unit_rows
    nheavy = heavy_ref.shape[1]
    per_line = LANES // rows
    scale = 1.0 / math.sqrt(DH)

    me_seq = lax.axis_index("seq")
    me_head = lax.axis_index("head")

    def seq_peer(step):
        return lax.rem(me_seq + step, n_seq)

    def head_peer(step):
        return lax.rem(me_head + step, n_head)

    pairs = (
        (refill_hbm, own_kv),
        (query_hbm, q_buf),
        (keys_hbm, k_buf),
        (lengths_hbm, lengths_ref),
        (heavy_hbm, heavy_ref),
        (req_hbm, req_ref),
        (head_hbm, head_ref),
        (dest_hbm, dest_ref),
        (values_hbm, v_buf),
        (acc_hbm, acc_ref),
    )
    loads = [pltpu.make_async_copy(*pair, load_sem.at[i]) for i, pair in enumerate(pairs)]
    for load in loads:
        load.start()

    barrier = pltpu.get_barrier_semaphore()
    for axis, me, size in (("seq", me_seq, n_seq), ("head", me_head, n_head)):
        for gap in range(1, size):

            @pl.when(me + gap < size)
            def _():
                pl.semaphore_signal(barrier, inc=1, device_id={axis: me + gap})

    @pl.when(me_seq + me_head > 0)
    def _():
        pl.semaphore_wait(barrier, me_seq + me_head)

    for gap in range(1, n_seq):

        @pl.when(me_seq >= gap)
        def _():
            pl.semaphore_signal(seq_ready.at[gap - 1], inc=1, device_id={"seq": me_seq - gap})

    for gap in range(1, n_head):

        @pl.when(me_head >= gap)
        def _():
            pl.semaphore_signal(head_ready, inc=1, device_id={"head": me_head - gap})

    loads[0].wait()

    stages = len(masks)
    span_rows = own_kv.shape[0] // chunks

    def mask_of(stage, chunk):
        return masks[stage] if low_first(chunk) else masks[stages - 1 - stage]

    def bit_of(place, mask):
        return lax.rem(lax.div(place, mask), 2)

    def held_at(stage):
        return own_kv if stage == 0 else kept_kv.at[stage - 1]

    def kv_copy(stage, chunk):
        mask = mask_of(stage, chunk)
        span = pl.ds(chunk * span_rows, span_rows)
        return pltpu.make_async_remote_copy(
            src_ref=held_at(stage).at[span],
            dst_ref=kv_buf.at[stage, span],
            send_sem=kv_send.at[0],
            recv_sem=kv_recv.at[stage, chunk],
            device_id={"seq": me_seq + mask - 2 * mask * bit_of(me_seq, mask)},
        )

    kv_copies = {(i, c): kv_copy(i, c) for i in range(stages) for c in range(chunks)}

    def kv_settle(stage, chunk):
        mask = mask_of(stage, chunk)
        kv_copies[stage, chunk].wait_recv()
        first, last = chunk * span_rows, (chunk + 1) * span_rows
        while first < last:
            tile = first // BLKTOK
            size = min(last, (tile + 1) * BLKTOK) - first
            span = pl.ds(first, size)
            steps = steps_along[tile // 2]
            origin = me_seq
            if low_first(chunk):
                low = lax.rem(me_seq, mask)
                origin = me_seq - low + lax.rem(low - lax.rem(steps, mask) + mask, mask)
            stays = bit_of(me_seq, mask) == bit_of(origin + steps, mask)
            after = jnp.where(stays, held_at(stage)[span], kv_buf[stage, span])
            if stage == stages - 1:
                recalled_ref[tile // 2, tile % 2, pl.ds(first % BLKTOK, size)] = after
            else:
                kept_kv[stage, span] = after
            first += size
        if stage < stages - 1:
            kv_copies[stage + 1, chunk].start()

    def kv_start(chunk, upward):
        @pl.when(bit_of(me_seq, mask_of(0, chunk)) == 1 - upward)
        def _():
            kv_copies[0, chunk].start()

    eager = lax.rem(me_head, 2) < EAGER

    @pl.when(eager)
    def _():
        for chunk in ORDER[:EARLY]:
            kv_start(chunk, 0)

    for load in loads[1:]:
        load.wait()
    owners = [dest_ref[0, j] for j in range(held)]
    steps_along = [lax.rem(owners[j] - me_seq + n_seq, n_seq) for j in range(held)]

    def tile_of(tile):
        return pl.ds(tile * BLKTOK, BLKTOK)

    q_rows = []
    for b in range(requests):
        line = q_buf[b : b + 1, :].astype(jnp.float32)
        for i in range(heads_local):
            q_rows.append(line[:, i * DH : (i + 1) * DH])
    q_all = jnp.concatenate(q_rows, axis=0).astype(jnp.bfloat16)

    contract = (((1,), (1,)), ((), ()))
    position = me_seq * seq_local + lax.broadcasted_iota(jnp.int32, (heads_local, seq_local), 1)
    token_block = lax.div(position, BLKTOK)
    cache_parts = []
    for b in range(requests):
        length = lengths_ref[b]
        keep = token_block >= lax.div(length - 1, BLKTOK) - (RECENT - 1)
        for n in range(nheavy):
            keep = keep | (token_block == heavy_ref[b, n])
        keep = keep & (position < length)
        seg_scores = []
        for g in range(kv_local):
            start = b * heads_local + g * per_group
            seg_scores.append(
                lax.dot_general(
                    q_all[start : start + per_group],
                    k_buf[b, :, g * DH : (g + 1) * DH],
                    contract,
                    preferred_element_type=jnp.float32,
                )
            )
        scores = jnp.concatenate(seg_scores, axis=0) * scale
        cache_parts.append(jnp.where(keep, scores, NEG_BIG))
    row_of = lax.broadcasted_iota(jnp.int32, (rows, BLKTOK), 0)
    segment_of = lax.div(row_of, per_group)
    unit_scores = []
    for u in range(held):
        member = segment_of == req_ref[u] * kv_local + head_ref[u]
        scores = (
            lax.dot_general(q_all, own_kv[tile_of(2 * u)], contract, preferred_element_type=jnp.float32)
            * scale
        )
        unit_scores.append(jnp.where(member, scores, NEG_BIG))

    cache_scores = jnp.concatenate(cache_parts, axis=0)
    best = jnp.max(cache_scores, axis=1, keepdims=True)
    for scores in unit_scores:
        best = jnp.maximum(best, jnp.max(scores, axis=1, keepdims=True))
    live = cache_scores > 0.5 * NEG_BIG
    cache_exp = jnp.where(live, jnp.exp(cache_scores - best), 0.0)
    block_sums = [
        jnp.sum(cache_exp[:, j * BLKTOK : (j + 1) * BLKTOK], axis=1, keepdims=True)
        for j in range(blocks_local)
    ]
    unit_exps = [
        jnp.where(scores > 0.5 * NEG_BIG, jnp.exp(scores - best), 0.0) for scores in unit_scores
    ]
    unit_sums = [jnp.sum(part, axis=1, keepdims=True) for part in unit_exps]
    total = functools.reduce(jnp.add, block_sums + unit_sums)

    columns = [best, total] + unit_sums
    lines = stat_buf.shape[1]
    columns += [jnp.zeros_like(best)] * (lines * per_line - len(columns))
    lane = lax.broadcasted_iota(jnp.int32, (LANES, LANES), 1)
    square = jnp.zeros((LANES, LANES), jnp.float32)
    for line in range(lines):
        column = jnp.concatenate(columns[line * per_line : (line + 1) * per_line], axis=0)
        square = jnp.where(lane == line, column, square)
    stat_buf[0] = square.T[:lines]

    cache_exp = cache_exp.astype(jnp.bfloat16)
    outs = []
    for b in range(requests):
        for g in range(kv_local):
            start = b * heads_local + g * per_group
            outs.append(
                jnp.dot(
                    cache_exp[start : start + per_group],
                    v_buf[b, :, g * DH : (g + 1) * DH],
                    preferred_element_type=jnp.float32,
                )
            )
    accum = jnp.concatenate(outs, axis=0)
    for u in range(held):
        accum = accum + jnp.dot(
            unit_exps[u].astype(jnp.bfloat16), own_kv[tile_of(2 * u + 1)], preferred_element_type=jnp.float32
        )
    part_buf[0] = accum.astype(jnp.bfloat16)


    def part_start(step):
        for buf, send, recv in (
            (stat_buf, stat_send, stat_recv),
            (part_buf, part_send, part_recv),
        ):
            pltpu.make_async_remote_copy(
                src_ref=buf.at[0],
                dst_ref=buf.at[step],
                send_sem=send.at[0],
                recv_sem=recv.at[0],
                device_id={"seq": seq_peer(step)},
            ).start()

    for gap in range(1, n_seq):

        @pl.when(me_seq == gap)
        def _():
            part_start(n_seq - gap)

    @pl.when(jnp.logical_not(eager))
    def _():
        for chunk in ORDER[:EARLY]:
            kv_start(chunk, 0)

    for chunk in ORDER[EARLY:]:
        kv_start(chunk, 0)

    for gap in reversed(range(1, n_seq)):

        @pl.when(me_seq > gap)
        def _():
            part_start(n_seq - gap)

    for gap in range(1, n_seq):

        @pl.when(me_seq + gap < n_seq)
        def _():
            pl.semaphore_wait(seq_ready.at[gap - 1], 1)
            part_start(gap)

        for chunk in ORDER:
            if mask_of(0, chunk) == gap:
                kv_start(chunk, 1)

    for chunk in SETTLE[:RELAYED]:
        kv_settle(0, chunk)
    await_all(stat_buf.at[pl.ds(1, n_seq - 1)], stat_recv)
    await_all(part_buf.at[pl.ds(1, n_seq - 1)], part_recv)

    def stat_of(index):
        line = stat_buf[:, index // per_line, :]
        shift = index % per_line * rows
        return pltpu.roll(line, LANES - shift, 1) if shift else line

    row_lane = lax.broadcasted_iota(jnp.int32, (n_seq, LANES), 1)
    bests = stat_of(0)
    weights = jnp.exp(bests - jnp.max(bests, axis=0, keepdims=True))
    row_total = jnp.sum(weights * stat_of(1), axis=0, keepdims=True)
    valid = row_lane[:1] < rows
    inverse = jnp.where(valid, 1.0 / jnp.where(valid, row_total, 1.0), 0.0)
    factors = weights * inverse
    fill = jnp.zeros((LANES - n_seq, LANES), jnp.float32)
    tall = jnp.concatenate([factors, fill], axis=0).T[:rows]
    joined = jnp.zeros((rows, DH), jnp.float32)
    for step in range(n_seq):
        joined = joined + part_buf[step].astype(jnp.float32) * tall[:, step : step + 1]

    width = heads_local * DH
    mine = pl.ds(pl.multiple_of(me_head * width, width), width)
    pieces = []
    for i in range(heads_local):
        pieces.append(
            jnp.concatenate(
                [
                    joined[b * heads_local + i : b * heads_local + i + 1]
                    for b in range(requests)
                ],
                axis=0,
            )
        )
    attn_ref[:, mine] = jnp.concatenate(pieces, axis=1).astype(jnp.bfloat16)

    tile_row = lax.broadcasted_iota(jnp.int32, (8, LANES), 0)
    tile_lane = lax.broadcasted_iota(jnp.int32, (8, LANES), 1)
    mass = jnp.zeros((8, LANES), jnp.float32)
    for j in range(blocks_local):
        share = block_sums[j] * tall[:, 0:1]
        for b in range(requests):
            of_request = share[b * heads_local : (b + 1) * heads_local]
            value = jnp.sum(of_request, axis=0, keepdims=True)
            mass = jnp.where((tile_row == b) & (tile_lane == j), value, mass)
    mass_buf[0] = mass

    @pl.when(me_head < n_head - 1)
    def _():
        pl.semaphore_wait(head_ready, n_head - 1 - me_head)

    for step in range(1, n_head):
        for src, dst, send, recv in (
            (attn_ref.at[:, mine], attn_ref.at[:, mine], attn_send, attn_recv),
            (mass_buf.at[0], mass_buf.at[step], mass_send, mass_recv),
        ):
            pltpu.make_async_remote_copy(
                src_ref=src,
                dst_ref=dst,
                send_sem=send.at[0],
                recv_sem=recv.at[0],
                device_id={"head": head_peer(step)},
            ).start()

    recall = jnp.zeros((1, held), jnp.float32)
    held_lane = lax.broadcasted_iota(jnp.int32, (1, held), 1)
    slot = lax.broadcasted_iota(jnp.int32, (n_seq, LANES), 0)
    for j in range(held):
        share = jnp.where(slot == steps_along[j], stat_of(2 + j) * factors, 0.0)
        value = jnp.sum(jnp.sum(share, axis=0, keepdims=True), axis=1, keepdims=True)
        recall = jnp.where(held_lane == j, value, recall)
    recall_ref[...] = recall

    for chunk in SETTLE[RELAYED:]:
        kv_settle(0, chunk)
    for stage in range(1, stages):
        for chunk in LAST:
            kv_settle(stage, chunk)

    others = attn_ref.at[:, pl.ds(0, (n_head - 1) * width)]
    await_all(others, attn_recv)
    await_all(mass_buf.at[pl.ds(1, n_head - 1)], mass_recv)
    mass = mass_buf[0]
    for step in range(1, n_head):
        mass = mass + mass_buf[step]
    block_ref[...] = acc_ref[...] + mass[:requests, :blocks_local]

    await_all(kv_buf, kv_send)
    await_all(stat_buf.at[pl.ds(1, n_seq - 1)], stat_send)
    await_all(part_buf.at[pl.ds(1, n_seq - 1)], part_send)
    await_all(others, attn_send)
    await_all(mass_buf.at[pl.ds(1, n_head - 1)], mass_send)


def put_out(*refs):
    sources, targets, sems = refs[:4], refs[4:8], refs[8]
    copies = [
        pltpu.make_async_copy(source, target, sems.at[i])
        for i, (source, target) in enumerate(zip(sources, targets))
    ]
    for copy in copies:
        copy.start()
    for copy in copies:
        copy.wait()


def on_device(
    query,
    cache_keys,
    cache_values,
    lengths,
    heavy,
    acc_scores,
    refill_kv,
    refill_dest,
    refill_req,
    refill_head,
):
    n_seq = lax.axis_size("seq")
    n_head = lax.axis_size("head")
    requests = query.shape[0]
    rows = query.size // DH
    held = refill_kv.shape[0]
    masks = []
    while 2 ** len(masks) < n_seq:
        masks.append(2 ** len(masks))
    tiles = (2 * held * BLKTOK, DH)
    lines = -(-(2 + held) // (LANES // rows))
    dma = pltpu.SemaphoreType.DMA
    hbm = pl.BlockSpec(memory_space=pltpu.HBM)
    vmem = pl.BlockSpec(memory_space=pltpu.VMEM)
    anywhere = pl.BlockSpec(memory_space=pl.ANY)
    results = pl.pallas_call(
        functools.partial(kernel, (n_seq, n_head, masks, CHUNKS)),
        out_shape=(
            pltpu.VMEM((requests, query.shape[1] * n_head), jnp.bfloat16),
            pltpu.VMEM(acc_scores.shape, jnp.float32),
            pltpu.VMEM(refill_kv.shape, jnp.bfloat16),
            pltpu.VMEM((1, held), jnp.float32),
        ),
        in_specs=[hbm] * 10,
        out_specs=(vmem,) * 4,
        scratch_shapes=[
            pltpu.SMEM(lengths.shape, jnp.int32),
            pltpu.SMEM(heavy.shape, jnp.int32),
            pltpu.SMEM((1, held), jnp.int32),
            pltpu.SMEM(refill_req.shape, jnp.int32),
            pltpu.SMEM(refill_head.shape, jnp.int32),
            pltpu.VMEM(acc_scores.shape, jnp.float32),
            pltpu.VMEM(query.shape, jnp.bfloat16),
            pltpu.VMEM(cache_keys.shape, jnp.bfloat16),
            pltpu.VMEM(cache_values.shape, jnp.bfloat16),
            pltpu.VMEM(tiles, jnp.bfloat16),
            pltpu.VMEM((len(masks),) + tiles, jnp.bfloat16),
            pltpu.VMEM((max(len(masks) - 1, 1),) + tiles, jnp.bfloat16),
            pltpu.VMEM((n_seq, rows, DH), jnp.bfloat16),
            pltpu.VMEM((n_seq, lines, LANES), jnp.float32),
            pltpu.VMEM((n_head, 8, LANES), jnp.float32),
            dma((10,)),
            dma((1,)),
            dma((len(masks), CHUNKS)),
            *[dma((1,))] * 8,
            pltpu.SemaphoreType.REGULAR((n_seq - 1,)),
            pltpu.SemaphoreType.REGULAR,
        ],
        compiler_params=pltpu.CompilerParams(
            collective_id=0, has_side_effects=True
        ),
    )(
        lengths,
        heavy,
        refill_dest.reshape(1, held),
        refill_req,
        refill_head,
        acc_scores,
        query,
        cache_keys,
        cache_values,
        refill_kv.reshape(tiles),
    )
    return pl.pallas_call(
        put_out,
        out_shape=tuple(jax.ShapeDtypeStruct(x.shape, x.dtype) for x in results),
        in_specs=[vmem] * 4,
        out_specs=(anywhere,) * 4,
        scratch_shapes=[dma((4,))],
        compiler_params=pltpu.CompilerParams(vmem_limit_bytes=VMEM_OUT),
    )(*results)


def solution(mesh):
    in_specs = (
        P("groups", "head"),
        P("groups", "seq", "head"),
        P("groups", "seq", "head"),
        P("groups"),
        P("groups", None),
        P("groups", "seq"),
        P(("groups", "seq", "head"), None, None, None),
        P(("groups", "seq", "head"), None),
        P(("groups", "seq", "head")),
        P(("groups", "seq", "head")),
    )
    out_specs = (
        P("groups", None),
        P("groups", "seq"),
        P(("groups", "seq", "head"), None, None, None),
        P(("groups", "seq", "head"), None),
    )
    return jax.shard_map(
        on_device, mesh=mesh, in_specs=in_specs, out_specs=out_specs, check_vma=False
    )
```

```python
import functools
import math

import jax
import jax.numpy as jnp
from jax import lax
from jax.experimental import pallas as pl
from jax.experimental.pallas import tpu as pltpu
from jax.sharding import PartitionSpec as P

DH = 128
BLKTOK = 128
RECENT = 2
CHUNKS = 4
PLACES = 4
EARLY = ((2, 2), (2, 2), (2, 2), (1, 4))
LOW_PARITY = 1
ORDER = (1, 0, 3, 2)
BEFORE = ((), (1, 3, 0, 2), (1, 3, 0, 2), ())
AFTER = ((0, 2, 1, 3), (), (), (1, 3, 0, 2))
LAST = (1, 3, 0, 2)
VMEM_OUT = 2**20
LANES = 128

NEG_BIG = -1e30


def low_first(chunk):
    return chunk % 2 == LOW_PARITY


def await_all(ref, sem):
    pltpu.make_async_copy(ref, ref, sem.at[0]).wait()


def kernel(
    dims,
    lengths_hbm,
    heavy_hbm,
    dest_hbm,
    req_hbm,
    head_hbm,
    acc_hbm,
    query_hbm,
    keys_hbm,
    values_hbm,
    refill_hbm,
    attn_ref,
    block_ref,
    recalled_ref,
    recall_ref,
    lengths_ref,
    heavy_ref,
    dest_ref,
    req_ref,
    head_ref,
    acc_ref,
    q_buf,
    k_buf,
    v_buf,
    own_kv,
    kv_buf,
    kept_kv,
    part_buf,
    stat_buf,
    mass_buf,
    load_sem,
    kv_send,
    kv_recv,
    part_send,
    part_recv,
    stat_send,
    stat_recv,
    attn_send,
    attn_recv,
    mass_send,
    mass_recv,
    seq_ready,
    head_ready,
):
    n_seq, n_head, masks, chunks = dims
    requests, seq_local = k_buf.shape[0], k_buf.shape[1]
    kv_local = k_buf.shape[2] // DH
    heads_local = q_buf.shape[1] // DH
    per_group = heads_local // kv_local
    rows = requests * heads_local
    blocks_local = seq_local // BLKTOK
    unit_rows = 2 * BLKTOK
    held = own_kv.shape[0] // unit_rows
    nheavy = heavy_ref.shape[1]
    per_line = LANES // rows
    scale = 1.0 / math.sqrt(DH)

    me_seq = lax.axis_index("seq")
    me_head = lax.axis_index("head")

    def seq_peer(step):
        return lax.rem(me_seq + step, n_seq)

    def head_peer(step):
        return lax.rem(me_head + step, n_head)

    pairs = (
        (refill_hbm, own_kv),
        (query_hbm, q_buf),
        (keys_hbm, k_buf),
        (lengths_hbm, lengths_ref),
        (heavy_hbm, heavy_ref),
        (req_hbm, req_ref),
        (head_hbm, head_ref),
        (dest_hbm, dest_ref),
        (values_hbm, v_buf),
        (acc_hbm, acc_ref),
    )
    loads = [pltpu.make_async_copy(*pair, load_sem.at[i]) for i, pair in enumerate(pairs)]
    for load in loads:
        load.start()

    barrier = pltpu.get_barrier_semaphore()
    for axis, me, size in (("seq", me_seq, n_seq), ("head", me_head, n_head)):
        for gap in range(1, size):

            @pl.when(me + gap < size)
            def _():
                pl.semaphore_signal(barrier, inc=1, device_id={axis: me + gap})

    @pl.when(me_seq + me_head > 0)
    def _():
        pl.semaphore_wait(barrier, me_seq + me_head)

    for gap in range(1, n_seq):

        @pl.when(me_seq >= gap)
        def _():
            pl.semaphore_signal(seq_ready.at[gap - 1], inc=1, device_id={"seq": me_seq - gap})

    for gap in range(1, n_head):

        @pl.when(me_head >= gap)
        def _():
            pl.semaphore_signal(head_ready, inc=1, device_id={"head": me_head - gap})

    loads[0].wait()

    stages = len(masks)
    span_rows = own_kv.shape[0] // chunks

    def mask_of(stage, chunk):
        return masks[stage] if low_first(chunk) else masks[stages - 1 - stage]

    def bit_of(place, mask):
        return lax.rem(lax.div(place, mask), 2)

    def held_at(stage):
        return own_kv if stage == 0 else kept_kv.at[stage - 1]

    def kv_copy(stage, chunk):
        mask = mask_of(stage, chunk)
        span = pl.ds(chunk * span_rows, span_rows)
        return pltpu.make_async_remote_copy(
            src_ref=held_at(stage).at[span],
            dst_ref=kv_buf.at[stage, span],
            send_sem=kv_send.at[0],
            recv_sem=kv_recv.at[stage, chunk],
            device_id={"seq": me_seq + mask - 2 * mask * bit_of(me_seq, mask)},
        )

    kv_copies = {(i, c): kv_copy(i, c) for i in range(stages) for c in range(chunks)}

    def kv_settle(stage, chunk):
        mask = mask_of(stage, chunk)
        kv_copies[stage, chunk].wait_recv()
        first, last = chunk * span_rows, (chunk + 1) * span_rows
        while first < last:
            tile = first // BLKTOK
            size = min(last, (tile + 1) * BLKTOK) - first
            span = pl.ds(first, size)
            steps = steps_along[tile // 2]
            origin = me_seq
            if low_first(chunk):
                low = lax.rem(me_seq, mask)
                origin = me_seq - low + lax.rem(low - lax.rem(steps, mask) + mask, mask)
            stays = bit_of(me_seq, mask) == bit_of(origin + steps, mask)
            after = jnp.where(stays, held_at(stage)[span], kv_buf[stage, span])
            if stage == stages - 1:
                recalled_ref[tile // 2, tile % 2, pl.ds(first % BLKTOK, size)] = after
            else:
                kept_kv[stage, span] = after
            first += size
        if stage < stages - 1:
            kv_copies[stage + 1, chunk].start()

    place = lax.rem(me_seq, PLACES)
    side = lax.rem(me_head, 2)

    def kv_down(early):
        for index, counts in enumerate(EARLY):
            for half, count in enumerate(counts):

                @pl.when((place == index) & (side == half))
                def _():
                    for chunk in ORDER[:count] if early else ORDER[count:]:
                        mask = mask_of(0, chunk)
                        if mask >= PLACES:
                            pl.when(bit_of(me_seq, mask) == 1)(kv_copies[0, chunk].start)
                        elif index & mask:
                            kv_copies[0, chunk].start()

    kv_down(True)

    for load in loads[1:]:
        load.wait()
    owners = [dest_ref[0, j] for j in range(held)]
    steps_along = [lax.rem(owners[j] - me_seq + n_seq, n_seq) for j in range(held)]

    def tile_of(tile):
        return pl.ds(tile * BLKTOK, BLKTOK)

    q_rows = []
    for b in range(requests):
        line = q_buf[b : b + 1, :].astype(jnp.float32)
        for i in range(heads_local):
            q_rows.append(line[:, i * DH : (i + 1) * DH])
    q_all = jnp.concatenate(q_rows, axis=0).astype(jnp.bfloat16)

    contract = (((1,), (1,)), ((), ()))
    position = me_seq * seq_local + lax.broadcasted_iota(jnp.int32, (heads_local, seq_local), 1)
    token_block = lax.div(position, BLKTOK)
    cache_parts = []
    for b in range(requests):
        length = lengths_ref[b]
        keep = token_block >= lax.div(length - 1, BLKTOK) - (RECENT - 1)
        for n in range(nheavy):
            keep = keep | (token_block == heavy_ref[b, n])
        keep = keep & (position < length)
        seg_scores = []
        for g in range(kv_local):
            start = b * heads_local + g * per_group
            seg_scores.append(
                lax.dot_general(
                    q_all[start : start + per_group],
                    k_buf[b, :, g * DH : (g + 1) * DH],
                    contract,
                    preferred_element_type=jnp.float32,
                )
            )
        scores = jnp.concatenate(seg_scores, axis=0) * scale
        cache_parts.append(jnp.where(keep, scores, NEG_BIG))
    row_of = lax.broadcasted_iota(jnp.int32, (rows, BLKTOK), 0)
    segment_of = lax.div(row_of, per_group)
    unit_scores = []
    for u in range(held):
        member = segment_of == req_ref[u] * kv_local + head_ref[u]
        scores = (
            lax.dot_general(q_all, own_kv[tile_of(2 * u)], contract, preferred_element_type=jnp.float32)
            * scale
        )
        unit_scores.append(jnp.where(member, scores, NEG_BIG))

    cache_scores = jnp.concatenate(cache_parts, axis=0)
    best = jnp.max(cache_scores, axis=1, keepdims=True)
    for scores in unit_scores:
        best = jnp.maximum(best, jnp.max(scores, axis=1, keepdims=True))
    live = cache_scores > 0.5 * NEG_BIG
    cache_exp = jnp.where(live, jnp.exp(cache_scores - best), 0.0)
    block_sums = [
        jnp.sum(cache_exp[:, j * BLKTOK : (j + 1) * BLKTOK], axis=1, keepdims=True)
        for j in range(blocks_local)
    ]
    unit_exps = [
        jnp.where(scores > 0.5 * NEG_BIG, jnp.exp(scores - best), 0.0) for scores in unit_scores
    ]
    unit_sums = [jnp.sum(part, axis=1, keepdims=True) for part in unit_exps]
    total = functools.reduce(jnp.add, block_sums + unit_sums)

    columns = [best, total] + unit_sums
    lines = stat_buf.shape[1]
    columns += [jnp.zeros_like(best)] * (lines * per_line - len(columns))
    lane = lax.broadcasted_iota(jnp.int32, (LANES, LANES), 1)
    square = jnp.zeros((LANES, LANES), jnp.float32)
    for line in range(lines):
        column = jnp.concatenate(columns[line * per_line : (line + 1) * per_line], axis=0)
        square = jnp.where(lane == line, column, square)
    stat_buf[0] = square.T[:lines]

    cache_exp = cache_exp.astype(jnp.bfloat16)
    outs = []
    for b in range(requests):
        for g in range(kv_local):
            start = b * heads_local + g * per_group
            outs.append(
                jnp.dot(
                    cache_exp[start : start + per_group],
                    v_buf[b, :, g * DH : (g + 1) * DH],
                    preferred_element_type=jnp.float32,
                )
            )
    accum = jnp.concatenate(outs, axis=0)
    for u in range(held):
        accum = accum + jnp.dot(
            unit_exps[u].astype(jnp.bfloat16), own_kv[tile_of(2 * u + 1)], preferred_element_type=jnp.float32
        )
    part_buf[0] = accum.astype(jnp.bfloat16)


    def part_start(step):
        for buf, send, recv in (
            (stat_buf, stat_send, stat_recv),
            (part_buf, part_send, part_recv),
        ):
            pltpu.make_async_remote_copy(
                src_ref=buf.at[0],
                dst_ref=buf.at[step],
                send_sem=send.at[0],
                recv_sem=recv.at[0],
                device_id={"seq": seq_peer(step)},
            ).start()

    for gap in range(1, n_seq):

        @pl.when(me_seq == gap)
        def _():
            part_start(n_seq - gap)

    kv_down(False)

    for gap in reversed(range(1, n_seq)):

        @pl.when(me_seq > gap)
        def _():
            part_start(n_seq - gap)

    for gap in range(1, n_seq):

        @pl.when(me_seq + gap < n_seq)
        def _():
            pl.semaphore_wait(seq_ready.at[gap - 1], 1)
            part_start(gap)

        if gap in masks:

            @pl.when(bit_of(me_seq, gap) == 0)
            def _():
                for chunk in ORDER:
                    if mask_of(0, chunk) == gap:
                        kv_copies[0, chunk].start()


    def relay(orders):
        for index, order in enumerate(orders):
            if not order:
                continue

            @pl.when(place == index)
            def _():
                for chunk in order:
                    kv_settle(0, chunk)

    relay(BEFORE)
    await_all(stat_buf.at[pl.ds(1, n_seq - 1)], stat_recv)
    await_all(part_buf.at[pl.ds(1, n_seq - 1)], part_recv)

    def stat_of(index):
        line = stat_buf[:, index // per_line, :]
        shift = index % per_line * rows
        return pltpu.roll(line, LANES - shift, 1) if shift else line

    row_lane = lax.broadcasted_iota(jnp.int32, (n_seq, LANES), 1)
    bests = stat_of(0)
    weights = jnp.exp(bests - jnp.max(bests, axis=0, keepdims=True))
    row_total = jnp.sum(weights * stat_of(1), axis=0, keepdims=True)
    valid = row_lane[:1] < rows
    inverse = jnp.where(valid, 1.0 / jnp.where(valid, row_total, 1.0), 0.0)
    factors = weights * inverse
    fill = jnp.zeros((LANES - n_seq, LANES), jnp.float32)
    tall = jnp.concatenate([factors, fill], axis=0).T[:rows]
    joined = jnp.zeros((rows, DH), jnp.float32)
    for step in range(n_seq):
        joined = joined + part_buf[step].astype(jnp.float32) * tall[:, step : step + 1]

    width = heads_local * DH
    mine = pl.ds(pl.multiple_of(me_head * width, width), width)
    pieces = []
    for i in range(heads_local):
        pieces.append(
            jnp.concatenate(
                [
                    joined[b * heads_local + i : b * heads_local + i + 1]
                    for b in range(requests)
                ],
                axis=0,
            )
        )
    attn_ref[:, mine] = jnp.concatenate(pieces, axis=1).astype(jnp.bfloat16)

    tile_row = lax.broadcasted_iota(jnp.int32, (8, LANES), 0)
    tile_lane = lax.broadcasted_iota(jnp.int32, (8, LANES), 1)
    mass = jnp.zeros((8, LANES), jnp.float32)
    for j in range(blocks_local):
        share = block_sums[j] * tall[:, 0:1]
        for b in range(requests):
            of_request = share[b * heads_local : (b + 1) * heads_local]
            value = jnp.sum(of_request, axis=0, keepdims=True)
            mass = jnp.where((tile_row == b) & (tile_lane == j), value, mass)
    mass_buf[0] = mass

    @pl.when(me_head < n_head - 1)
    def _():
        pl.semaphore_wait(head_ready, n_head - 1 - me_head)

    for step in range(1, n_head):
        for src, dst, send, recv in (
            (attn_ref.at[:, mine], attn_ref.at[:, mine], attn_send, attn_recv),
            (mass_buf.at[0], mass_buf.at[step], mass_send, mass_recv),
        ):
            pltpu.make_async_remote_copy(
                src_ref=src,
                dst_ref=dst,
                send_sem=send.at[0],
                recv_sem=recv.at[0],
                device_id={"head": head_peer(step)},
            ).start()

    recall = jnp.zeros((1, held), jnp.float32)
    held_lane = lax.broadcasted_iota(jnp.int32, (1, held), 1)
    slot = lax.broadcasted_iota(jnp.int32, (n_seq, LANES), 0)
    for j in range(held):
        share = jnp.where(slot == steps_along[j], stat_of(2 + j) * factors, 0.0)
        value = jnp.sum(jnp.sum(share, axis=0, keepdims=True), axis=1, keepdims=True)
        recall = jnp.where(held_lane == j, value, recall)
    recall_ref[...] = recall

    relay(AFTER)
    for stage in range(1, stages):
        for chunk in LAST:
            kv_settle(stage, chunk)

    others = attn_ref.at[:, pl.ds(0, (n_head - 1) * width)]
    await_all(others, attn_recv)
    await_all(mass_buf.at[pl.ds(1, n_head - 1)], mass_recv)
    mass = mass_buf[0]
    for step in range(1, n_head):
        mass = mass + mass_buf[step]
    block_ref[...] = acc_ref[...] + mass[:requests, :blocks_local]

    await_all(kv_buf, kv_send)
    await_all(stat_buf.at[pl.ds(1, n_seq - 1)], stat_send)
    await_all(part_buf.at[pl.ds(1, n_seq - 1)], part_send)
    await_all(others, attn_send)
    await_all(mass_buf.at[pl.ds(1, n_head - 1)], mass_send)


def put_out(*refs):
    sources, targets, sems = refs[:4], refs[4:8], refs[8]
    copies = [
        pltpu.make_async_copy(source, target, sems.at[i])
        for i, (source, target) in enumerate(zip(sources, targets))
    ]
    for copy in copies:
        copy.start()
    for copy in copies:
        copy.wait()


def on_device(
    query,
    cache_keys,
    cache_values,
    lengths,
    heavy,
    acc_scores,
    refill_kv,
    refill_dest,
    refill_req,
    refill_head,
):
    n_seq = lax.axis_size("seq")
    n_head = lax.axis_size("head")
    requests = query.shape[0]
    rows = query.size // DH
    held = refill_kv.shape[0]
    masks = []
    while 2 ** len(masks) < n_seq:
        masks.append(2 ** len(masks))
    tiles = (2 * held * BLKTOK, DH)
    lines = -(-(2 + held) // (LANES // rows))
    dma = pltpu.SemaphoreType.DMA
    hbm = pl.BlockSpec(memory_space=pltpu.HBM)
    vmem = pl.BlockSpec(memory_space=pltpu.VMEM)
    anywhere = pl.BlockSpec(memory_space=pl.ANY)
    results = pl.pallas_call(
        functools.partial(kernel, (n_seq, n_head, masks, CHUNKS)),
        out_shape=(
            pltpu.VMEM((requests, query.shape[1] * n_head), jnp.bfloat16),
            pltpu.VMEM(acc_scores.shape, jnp.float32),
            pltpu.VMEM(refill_kv.shape, jnp.bfloat16),
            pltpu.VMEM((1, held), jnp.float32),
        ),
        in_specs=[hbm] * 10,
        out_specs=(vmem,) * 4,
        scratch_shapes=[
            pltpu.SMEM(lengths.shape, jnp.int32),
            pltpu.SMEM(heavy.shape, jnp.int32),
            pltpu.SMEM((1, held), jnp.int32),
            pltpu.SMEM(refill_req.shape, jnp.int32),
            pltpu.SMEM(refill_head.shape, jnp.int32),
            pltpu.VMEM(acc_scores.shape, jnp.float32),
            pltpu.VMEM(query.shape, jnp.bfloat16),
            pltpu.VMEM(cache_keys.shape, jnp.bfloat16),
            pltpu.VMEM(cache_values.shape, jnp.bfloat16),
            pltpu.VMEM(tiles, jnp.bfloat16),
            pltpu.VMEM((len(masks),) + tiles, jnp.bfloat16),
            pltpu.VMEM((max(len(masks) - 1, 1),) + tiles, jnp.bfloat16),
            pltpu.VMEM((n_seq, rows, DH), jnp.bfloat16),
            pltpu.VMEM((n_seq, lines, LANES), jnp.float32),
            pltpu.VMEM((n_head, 8, LANES), jnp.float32),
            dma((10,)),
            dma((1,)),
            dma((len(masks), CHUNKS)),
            *[dma((1,))] * 8,
            pltpu.SemaphoreType.REGULAR((n_seq - 1,)),
            pltpu.SemaphoreType.REGULAR,
        ],
        compiler_params=pltpu.CompilerParams(
            collective_id=0, has_side_effects=True
        ),
    )(
        lengths,
        heavy,
        refill_dest.reshape(1, held),
        refill_req,
        refill_head,
        acc_scores,
        query,
        cache_keys,
        cache_values,
        refill_kv.reshape(tiles),
    )
    return pl.pallas_call(
        put_out,
        out_shape=tuple(jax.ShapeDtypeStruct(x.shape, x.dtype) for x in results),
        in_specs=[vmem] * 4,
        out_specs=(anywhere,) * 4,
        scratch_shapes=[dma((4,))],
        compiler_params=pltpu.CompilerParams(vmem_limit_bytes=VMEM_OUT),
    )(*results)


def solution(mesh):
    in_specs = (
        P("groups", "head"),
        P("groups", "seq", "head"),
        P("groups", "seq", "head"),
        P("groups"),
        P("groups", None),
        P("groups", "seq"),
        P(("groups", "seq", "head"), None, None, None),
        P(("groups", "seq", "head"), None),
        P(("groups", "seq", "head")),
        P(("groups", "seq", "head")),
    )
    out_specs = (
        P("groups", None),
        P("groups", "seq"),
        P(("groups", "seq", "head"), None, None, None),
        P(("groups", "seq", "head"), None),
    )
    return jax.shard_map(
        on_device, mesh=mesh, in_specs=in_specs, out_specs=out_specs, check_vma=False
    )
```
